256 devices in a mesh: ens: 4 (over x), batch: 16 (over z, core), cols: 4 (over y).
Axes of the slice: x: 4, y: 4, z: 8, core: 2. Of those that a mesh axis runs over, the one named last changes fastest.
Arguments:
- grad_up: bfloat16 [64, 1280, 5120], P(('ens', 'batch'), None, 'cols'), parts along dimension 0, may hold values from -0.875 to 0.875
- grad_down: bfloat16 [64, 5120, 1280], P(('ens', 'batch'), 'cols'), parts along dimension 0, may hold values from -0.875 to 0.875
- grad_norm: bfloat16 [64, 1280], P(('ens', 'batch')), parts along dimension 0, may hold values from -8 to 8
- grad_bias: bfloat16 [64, 1280], P(('ens', 'batch')), parts along dimension 0, may hold values from -8 to 8
- weight_up: float32 [5120, 5120], P(('ens', 'batch'), 'cols'), parts along dimension 0, may hold values from -0.25 to 0.25
- weight_down: float32 [20480, 1280], P(('ens', 'cols'), 'batch'), parts along dimension 0, may hold values from -0.125 to 0.125
- weight_norm: float32 [5120], P(('ens', 'batch')), parts along dimension 0, may hold values from 0.25 to 1.75
- weight_bias: float32 [5120], P(('ens', 'batch')), parts along dimension 0, may hold values from -3 to 3
Outputs:
- copy_up: bfloat16 [5120, 5120], P('ens', 'cols'), parts along dimension 0
- copy_down: bfloat16 [20480, 1280], P(('ens', 'cols')), parts along dimension 0
- copy_norm: bfloat16 [5120], P('ens'), parts along dimension 0
- copy_bias: bfloat16 [5120], P('ens'), parts along dimension 0
- new_up: float32 [5120, 5120], P(('ens', 'batch'), 'cols'), parts along dimension 0
- new_down: float32 [20480, 1280], P(('ens', 'cols'), 'batch'), parts along dimension 0
- new_norm: float32 [5120], P(('ens', 'batch')), parts along dimension 0
- new_bias: float32 [5120], P(('ens', 'batch')), parts along dimension 0
The draws below stay inside these ranges and needn't reach their ends.
There are 4 independent parts, one for each index of `ens`. The reference program is written for one: setup_inputs(seed, part) draws one part's arguments, and reference() takes and returns one part's arrays. A program takes and returns all parts, laid end to end along the dimension named above; each array names one. Nothing has to cross between parts.
All inputs are finite; a program needn't handle non-finite values.
Results may differ from the reference program's by a relative error of at most 0.014.
Values may be sent and summed in bfloat16 or wider, within the bound.
A program may use at most 128 MiB of HBM per device.

```python
import jax
import jax.numpy as jnp
from jax import lax

WIDTH = 1280
INNER = 5120
REPLICAS = 16


def strengthened(array, key, source, target, shards_of, factor):
    def block_of(axis_at):
        return (jnp.arange(array.shape[axis_at]) // (array.shape[axis_at] // shards_of)).reshape((-1,) + (1,) * (array.ndim - 1 - axis_at))

    one_side = jax.random.permutation(key, shards_of)[block_of(target)]
    second = (block_of(target) + shards_of // 2) % shards_of
    return jnp.where((block_of(source) == one_side) | (block_of(source) == second), factor * array, array)


def block_levels(own_key, dims, cuts, low, top_value):
    def one(dim, shards_of):
        draws = jax.random.uniform(jax.random.fold_in(jax.random.fold_in(own_key, 6), dim), (shards_of,), jnp.float32, low / len(cuts), top_value / len(cuts))
        return jnp.repeat(jnp.exp(draws), dims[dim] // shards_of).reshape((-1,) + (1,) * (len(dims) - dim - 1))

    loudness = one(*cuts[0])
    for cut in cuts[1:]:
        loudness = loudness * one(*cut)
    return loudness


def normal_values(rng, extent, spread, bound, cuts=(), kind=jnp.bfloat16):
    values = spread * jax.random.normal(rng, extent, jnp.float32)
    if cuts:
        values = values * block_levels(rng, extent, cuts, -0.22, 0.18)
    return jnp.clip(values, -bound, bound).astype(kind)


def bell_draw_with(rng, extent, spread, reach, split, heavy, kind=jnp.bfloat16):
    values = spread * jax.random.normal(rng, extent, jnp.float32)
    if split:
        values = values * block_levels(rng, extent, split, -0.22, 0.18)
    return jnp.clip(strengthened(values, jax.random.fold_in(rng, 3), *heavy), -reach, reach).astype(kind)


def setup_inputs(seed: int = 0, part: int = 0) -> dict:
    streams_of = jax.random.split(jax.random.key(seed), 9)
    part_keys = jax.random.split(jax.random.fold_in(streams_of[8], part), 9)
    grad_up = bell_draw_with(part_keys[0], (REPLICAS, WIDTH, INNER), 0.1, 0.875, ((0, 16), (2, 4)), (0, 1, 16, 2.0))
    grad_down = bell_draw_with(part_keys[1], (REPLICAS, INNER, WIDTH), 0.1, 0.875, ((0, 16), (1, 4)), (0, 2, 16, 2.0))
    grad_norm = bell_draw_with(part_keys[2], (REPLICAS, WIDTH), 1.0, 8.0, ((0, 16),), (0, 1, 16, 2.0))
    grad_bias = bell_draw_with(part_keys[3], (REPLICAS, WIDTH), 1.0, 8.0, ((0, 16),), (0, 1, 16, 2.0))
    weight_up = bell_draw_with(part_keys[4], (WIDTH, INNER), WIDTH ** -0.5, 0.25, ((0, 16), (1, 4)), (1, 0, 16, 2.0), jnp.float32)
    weight_down = bell_draw_with(part_keys[5], (INNER, WIDTH), INNER ** -0.5, 0.125, ((0, 4), (1, 16)), (0, 1, 16, 2.0), jnp.float32)
    weight_norm = jnp.clip(1.0 + 0.15 * jax.random.normal(part_keys[6], (WIDTH,), jnp.float32), 0.25, 1.75)
    weight_bias = normal_values(part_keys[7], (WIDTH,), 0.5, 3.0, ((0, 16),), jnp.float32)
    return {"grad_up": grad_up, "grad_down": grad_down, "grad_norm": grad_norm, "grad_bias": grad_bias, "weight_up": weight_up, "weight_down": weight_down, "weight_norm": weight_norm, "weight_bias": weight_bias}


learn_rate = 0.4

def reference(grad_up, grad_down, grad_norm, grad_bias, weight_up, weight_down, weight_norm, weight_bias):
    mean_up = lax.optimization_barrier(jnp.sum(grad_up.astype(jnp.float32), axis=0)) * REPLICAS ** (-0.5)
    mean_down = lax.optimization_barrier(jnp.sum(grad_down.astype(jnp.float32), axis=0)) * REPLICAS ** (-0.5)
    mean_norm = lax.optimization_barrier(jnp.sum(grad_norm.astype(jnp.float32), axis=0)) * REPLICAS ** (-0.5)
    mean_bias = lax.optimization_barrier(jnp.sum(grad_bias.astype(jnp.float32), axis=0)) * REPLICAS ** (-0.5)
    ratio_up = jnp.sqrt(lax.optimization_barrier(jnp.sum(weight_up * weight_up, axis=1, keepdims=True))) * lax.rsqrt(lax.optimization_barrier(jnp.sum(mean_up * mean_up, axis=1, keepdims=True)) + 1e-06)
    mean_up = mean_up * ratio_up
    ratio_down = jnp.sqrt(lax.optimization_barrier(jnp.sum(weight_down * weight_down, axis=0, keepdims=True))) * lax.rsqrt(lax.optimization_barrier(jnp.sum(mean_down * mean_down, axis=0, keepdims=True)) + 1e-06)
    mean_down = mean_down * ratio_down
    new_up = weight_up - learn_rate * mean_up
    new_down = weight_down - learn_rate * mean_down
    new_norm = weight_norm - learn_rate * mean_norm
    new_bias = weight_bias - learn_rate * mean_bias
    copy_up = new_up.astype(jnp.bfloat16)
    copy_down = new_down.astype(jnp.bfloat16)
    copy_norm = new_norm.astype(jnp.bfloat16)
    copy_bias = new_bias.astype(jnp.bfloat16)
    return (copy_up, copy_down, copy_norm, copy_bias, new_up, new_down, new_norm, new_bias)
```

```python
import functools

import jax
import jax.numpy as jnp
from jax import lax
from jax.experimental import pallas as pl
from jax.experimental.pallas import tpu as pltpu
from jax.sharding import Mesh
from jax.sharding import PartitionSpec as P

AXES = ("ens", "z", "core", "cols")
RATE = 0.4
LANES = 128
F32 = jnp.float32
BF16 = jnp.bfloat16


def cut(rows):
    parts, at = [], 0
    for size in (32, 32, 16):
        if at < rows:
            parts.append((at, min(size, rows - at)))
            at += size
    return parts


def kernel(
    dims,
    gu, gd, gn, gb, wu, wd, wn, wb,
    cu, cd, cn, cb, nu, nd, nn, nb,
    raw, g_u, g_d, pair_u, pair_d, rcv_u, rcv_d, w_u, w_d, fin_u, fin_d, full_d,
    slope, own, vin, vw, vplace, vown, vpair, vslot, vfull, sems,
):
    ring, cols, rows, wide = dims
    z, core, y = lax.axis_index("z"), lax.axis_index("core"), lax.axis_index("cols")
    other = 1 - core
    far, near = ring // 2, ring - 1 - ring // 2
    mean_rate = (ring * 2) ** -0.5
    place = z * 2 + core
    count = [0]
    sent = []

    def new_sem():
        count[0] += 1
        return sems.at[count[0] - 1]

    def at_z(shift):
        return lax.rem(z + (shift + ring), ring)

    def fetch(src, dst):
        copy = pltpu.make_async_copy(src, dst, new_sem())
        copy.start()
        return copy

    def send(src, dst, **where):
        copy = pltpu.make_async_remote_copy(
            src_ref=src, dst_ref=dst, send_sem=new_sem(), recv_sem=new_sem(),
            device_id=where, device_id_type=pl.DeviceIdType.MESH,
        )
        copy.start()
        sent.append(copy)
        return copy

    def block(zd, part, r0, n):
        return pl.ds(pl.multiple_of((zd * 2 + part) * rows + r0, 16), n)

    shifts = [far]
    for d in range(near, 0, -1):
        shifts += [d, -d]
    shifts.append(0)
    slot_of = {s: k for k, s in enumerate(shifts)}
    slot_of[-far] = slot_of[far]

    loads_mine, loads_other = [], []
    for s in shifts:
        zd = at_z(s)
        for part, out in ((other, loads_other), (core, loads_mine)):
            here = block(zd, part, 0, rows)
            out.append(fetch(gu.at[here], g_u.at[here]))
    small = [
        fetch(gn, vin.at[0]), fetch(gb, vin.at[1]), fetch(wn, vw.at[0]), fetch(wb, vw.at[1]),
    ]
    load_raw = fetch(gd, raw)
    load_w = [fetch(wu, w_u), fetch(wd, w_d)]

    barrier = pltpu.get_barrier_semaphore()
    peers = [{"core": other}, {"z": at_z(1)}, {"z": at_z(-1)}]
    others_y = [lax.rem(y + k, cols) for k in range(1, cols)]
    peers += [{"cols": o} for o in others_y]
    for peer in peers:
        pl.semaphore_signal(barrier, inc=1, device_id=peer, device_id_type=pl.DeviceIdType.MESH)
    pl.semaphore_wait(barrier, len(peers))

    mats = {
        "u": dict(g=g_u, pair=pair_u, rcv=rcv_u, w=w_u, fin=fin_u, full=cu, new=nu, k=0),
        "d": dict(g=g_d, pair=pair_d, rcv=rcv_d, w=w_d, fin=fin_d, full=full_d, new=nd, k=1),
    }

    def swap(name):
        m = mats[name]
        m["swaps"] = []
        for k, s in enumerate(shifts):
            if name == "u":
                loads_other[k].wait()
            zd = at_z(s)
            m["swaps"].append(
                send(m["g"].at[block(zd, other, 0, rows)], m["pair"].at[zd], core=other)
            )
        m["ready"] = set()

    def pair_sum(m, shift, r0, n):
        k = slot_of[shift]
        if k not in m["ready"]:
            if m is mats["u"]:
                loads_mine[k].wait()
            m["swaps"][k].wait_recv()
            m["ready"].add(k)
        zd = at_z(shift)
        mine = m["g"][block(zd, core, r0, n), :].astype(F32)
        return mine + m["pair"][zd, pl.ds(r0, n), :].astype(F32)

    flows = []
    for name, flip in (("u", 0), ("d", 1)):
        for i, (r0, n) in enumerate(cut(rows)):
            reach = (near, far) if (i + flip) % 2 == 0 else (far, near)
            flows.append(dict(m=name, r0=r0, n=n, reach=reach, rs={}, ag={}, to={}))

    def of(name):
        return [f for f in flows if f["m"] == name]

    def scatter(name, step):
        m = mats[name]
        for f in of(name):
            r0, n = f["r0"], f["n"]
            for d, sign in ((1, -1), (0, 1)):
                reach = f["reach"][d]
                if step > reach:
                    continue
                shift = sign * (reach - step + 1)
                if abs(shift) == far:
                    shift = far
                total = pair_sum(m, shift, r0, n)
                if step > 1:
                    f["rs"][d, step - 1].wait_recv()
                    total += m["rcv"][d, step - 2, pl.ds(r0, n), :].astype(F32)
                zd = at_z(shift)
                m["pair"][zd, pl.ds(r0, n), :] = total.astype(BF16)
                f["rs"][d, step] = send(
                    m["pair"].at[zd, pl.ds(r0, n)],
                    m["rcv"].at[d, step - 1, pl.ds(r0, n)],
                    z=at_z(sign),
                )

    def folded(x):
        out = x[:, :LANES]
        for j in range(1, x.shape[1] // LANES):
            out += x[:, j * LANES : (j + 1) * LANES]
        return out

    def share_with_cols(table, k, r0, n):
        return [
            send(table.at[k, y, pl.ds(r0, n)], table.at[k, y, pl.ds(r0, n)], cols=o)
            for o in others_y
        ]

    def finish_sum(name):
        m = mats[name]
        for f in of(name):
            r0, n = f["r0"], f["n"]
            total = pair_sum(m, 0, r0, n)
            for d in (1, 0):
                reach = f["reach"][d]
                f["rs"][d, reach].wait_recv()
                total += m["rcv"][d, reach - 1, pl.ds(r0, n), :].astype(F32)
            mean = total * mean_rate
            m["fin"][pl.ds(r0, n), :] = mean
            slope[m["k"], y, pl.ds(r0, n), :] = folded(mean * mean)
            f["sizes"] = share_with_cols(slope, m["k"], r0, n)

    def size_of(table, k, r0, n):
        total = table[k, 0, pl.ds(r0, n), :]
        for j in range(1, cols):
            total += table[k, j, pl.ds(r0, n), :]
        return jnp.sum(total, axis=1, keepdims=True)

    def update(name):
        m = mats[name]
        for c in m.pop("own_sizes"):
            c.wait_recv()
        for f in of(name):
            r0, n = f["r0"], f["n"]
            for c in f["sizes"]:
                c.wait_recv()
            ratio = jnp.sqrt(size_of(own, m["k"], r0, n)) * lax.rsqrt(
                size_of(slope, m["k"], r0, n) + 1e-06
            )
            new = m["w"][pl.ds(r0, n), :] - RATE * (m["fin"][pl.ds(r0, n), :] * ratio)
            m["new"][pl.ds(r0, n), :] = new
            here = m["full"].at[block(z, core, r0, n)]
            here[...] = new.astype(BF16)
            for d, sign in ((1, -1), (0, 1)):
                f["ag"][d, 1] = send(here, here, z=at_z(sign))
            f["to"][0, 0] = send(here, here, core=other)

    def pass_on(name, step):
        m = mats[name]
        for f in of(name):
            for d, sign in ((1, -1), (0, 1)):
                reach = f["reach"][d]
                if step > reach:
                    continue
                f["ag"][d, step].wait_recv()
                here = m["full"].at[block(at_z(-sign * step), core, f["r0"], f["n"])]
                if step < reach:
                    f["ag"][d, step + 1] = send(here, here, z=at_z(sign))
                f["to"][d, step] = send(here, here, core=other)

    def all_here(name):
        for f in of(name):
            for copy in f["to"].values():
                copy.wait_recv()

    def vectors_out():
        for copy in small:
            copy.wait()
        vplace[...] = jnp.zeros_like(vplace)
        for v in range(2):
            vplace[pl.ds(v, 1), pl.ds(0, rows)] = vw[v]
        placed = pltpu.roll(vplace[...], place * rows, 1)
        for v in range(2):
            vown[v] = placed[v : v + 1, :] - (RATE * mean_rate) * vin[v].astype(F32)
        return send(vown.at[other], vpair, core=other)

    vec = {}

    def vectors_ring(step):
        if step == 1:
            vec["swap"].wait_recv()
            vslot[z] = vown[core] + vpair[...]
        for d, sign in ((1, -1), (0, 1)):
            reach = (near, far)[d]
            if step > 1 and step - 1 <= reach:
                vec[d, step - 1].wait_recv()
            if step <= reach:
                here = vslot.at[at_z(-sign * (step - 1))]
                vec[d, step] = send(here, here, z=at_z(sign))

    def vectors_sum():
        total = vslot[0]
        for k in range(1, ring):
            total += vslot[k]
        vfull[core] = total
        vec["full"] = send(vfull.at[core], vfull.at[core], core=other)

    def vectors_in():
        vec["full"].wait_recv()
        back = lax.rem(ring * 2 - place, ring * 2) * rows
        for v, (c_ref, n_ref) in enumerate(((cn, nn), (cb, nb))):
            c_ref[...] = vfull[v].astype(BF16)
            vplace[pl.ds(v, 1), :] = vfull[v]
        turned = pltpu.roll(vplace[...], back, 1)
        for v, n_ref in enumerate((nn, nb)):
            n_ref[...] = turned[v : v + 1, :rows]

    def turn_in():
        load_raw.wait()

        def slab(j, _):
            here = pl.ds(pl.multiple_of(j * LANES, LANES), LANES)
            g_d[here, :] = raw[:, here].T
            return 0

        lax.fori_loop(0, ring * 2 * rows // LANES, slab, 0)

    def turn_out():
        def slab(j, _):
            here = pl.ds(pl.multiple_of(j * LANES, LANES), LANES)
            cd[:, here] = full_d[here, :].T
            return 0

        lax.fori_loop(0, ring * 2 * rows // LANES, slab, 0)

    def own_sizes():
        for copy in load_w:
            copy.wait()
        for name in ("u", "d"):
            m = mats[name]
            w = m["w"][...]
            own[m["k"], y] = folded(w * w)
            m["own_sizes"] = share_with_cols(own, m["k"], 0, rows)

    swap("u")
    scatter("u", 1)
    vec["swap"] = vectors_out()
    turn_in()
    swap("d")
    vectors_ring(1)
    own_sizes()
    steps = far
    for s in range(2, steps):
        scatter("u", s)
        vectors_ring(s)
    scatter("d", 1)
    if steps > 1:
        scatter("u", steps)
        vectors_ring(steps)
    if steps > 1:
        scatter("d", 2)
    finish_sum("u")
    for s in range(3, steps + 1):
        scatter("d", s)
    vectors_ring(steps + 1)
    vectors_sum()
    update("u")
    finish_sum("d")
    vectors_in()
    pass_on("u", 1)
    update("d")
    pass_on("d", 1)
    for s in range(2, steps):
        pass_on("u", s)
        pass_on("d", s)
    if steps > 1:
        pass_on("d", steps)
        pass_on("u", steps)
    all_here("d")
    turn_out()
    all_here("u")
    for copy in sent:
        copy.wait_send()


def per_device(ring, cols, grad_up, grad_down, grad_norm, grad_bias, *weights):
    weight_up, weight_down, weight_norm, weight_bias = weights
    rows, wide = weight_up.shape
    total = ring * 2 * rows
    any_spec = pl.BlockSpec(memory_space=pl.ANY)
    vmem = pl.BlockSpec(memory_space=pltpu.VMEM)
    shape = jax.ShapeDtypeStruct
    outs = (
        shape((total, wide), BF16), shape((wide, total), BF16),
        shape((1, total), BF16), shape((1, total), BF16),
        shape((rows, wide), F32), shape((rows, wide), F32),
        shape((1, rows), F32), shape((1, rows), F32),
    )
    far = ring // 2
    scratch = [
        pltpu.VMEM((wide, total), BF16),
        pltpu.VMEM((total, wide), BF16), pltpu.VMEM((total, wide), BF16),
        pltpu.VMEM((ring, rows, wide), BF16), pltpu.VMEM((ring, rows, wide), BF16),
        pltpu.VMEM((2, far, rows, wide), BF16), pltpu.VMEM((2, far, rows, wide), BF16),
        pltpu.VMEM((rows, wide), F32), pltpu.VMEM((rows, wide), F32),
        pltpu.VMEM((rows, wide), F32), pltpu.VMEM((rows, wide), F32),
        pltpu.VMEM((total, wide), BF16),
        pltpu.VMEM((2, cols, rows, LANES), F32), pltpu.VMEM((2, cols, rows, LANES), F32),
        pltpu.VMEM((2, 1, total), BF16), pltpu.VMEM((2, 1, rows), F32),
        pltpu.VMEM((8, total), F32), pltpu.VMEM((2, 1, total), F32),
        pltpu.VMEM((1, total), F32), pltpu.VMEM((ring, 1, total), F32),
        pltpu.VMEM((2, 1, total), F32),
        pltpu.SemaphoreType.DMA((448,)),
    ]
    got = pl.pallas_call(
        functools.partial(kernel, (ring, cols, rows, wide)),
        out_shape=outs,
        in_specs=[any_spec] * 8,
        out_specs=[vmem] * 8,
        scratch_shapes=scratch,
        compiler_params=pltpu.CompilerParams(
            collective_id=0, has_side_effects=True, vmem_limit_bytes=60 * 2**20
        ),
        name="step",
    )(
        grad_up[0], grad_down[0], grad_norm, grad_bias,
        weight_up, weight_down.T, weight_norm[None], weight_bias[None],
    )
    copy_up, copy_down, copy_norm, copy_bias, new_up, new_down, new_norm, new_bias = got
    return (
        copy_up, copy_down, copy_norm[0], copy_bias[0],
        new_up, new_down.T, new_norm[0], new_bias[0],
    )


def solution(mesh):
    ring, cols = mesh.shape["batch"] // 2, mesh.shape["cols"]
    finer = Mesh(mesh.devices.reshape(mesh.shape["ens"], ring, 2, cols), AXES)
    batch = ("z", "core")
    all_of = ("ens", "z", "core")
    placed = (
        P(all_of, None, "cols"), P(all_of, "cols", None), P(all_of, None), P(all_of, None),
        P(all_of, "cols"), P(("ens", "cols"), batch), P(all_of), P(all_of),
    )
    return jax.shard_map(
        functools.partial(per_device, ring, cols),
        mesh=finer,
        in_specs=placed,
        out_specs=(
            P("ens", "cols"), P(("ens", "cols"), None), P("ens"), P("ens"),
            P(all_of, "cols"), P(("ens", "cols"), batch), P(all_of), P(all_of),
        ),
        check_vma=False,
    )
```

```python
import functools

import jax
import jax.numpy as jnp
from jax import lax
from jax.experimental import pallas as pl
from jax.experimental.pallas import tpu as pltpu
from jax.sharding import Mesh
from jax.sharding import PartitionSpec as P

AXES = ("ens", "z", "core", "cols")
RATE = 0.4
VL = 52
LANES = 128
F32 = jnp.float32
BF16 = jnp.bfloat16


def cut(rows):
    parts, at = [], 0
    for size in (32, 32, 16):
        if at < rows:
            parts.append((at, min(size, rows - at)))
            at += size
    return parts


def kernel(
    dims,
    gu, gd, gn, gb, wu, wd, wn, wb,
    cu, full_d, cn, cb, nu, nd, nn, nb,
    raw, g_u, g_d, pair_u, pair_d, rcv_u, rcv_d, w_u, w_d, fin_u, fin_d,
    slope, own, vin, vw, vplace, vown, vpair, vslot, vfull, sems,
):
    ring, cols, rows, wide = dims
    z, core, y = lax.axis_index("z"), lax.axis_index("core"), lax.axis_index("cols")
    other = 1 - core
    far, near = ring // 2, ring - 1 - ring // 2
    mean_rate = (ring * 2) ** -0.5
    place = z * 2 + core
    count = [0]
    sent = []

    def new_sem():
        count[0] += 1
        return sems.at[count[0] - 1]

    def at_z(shift):
        return lax.rem(z + (shift + ring), ring)

    def fetch(src, dst):
        copy = pltpu.make_async_copy(src, dst, new_sem())
        copy.start()
        return copy

    def send(src, dst, **where):
        copy = pltpu.make_async_remote_copy(
            src_ref=src, dst_ref=dst, send_sem=new_sem(), recv_sem=new_sem(),
            device_id=where, device_id_type=pl.DeviceIdType.MESH,
        )
        copy.start()
        sent.append(copy)
        return copy

    def block(zd, part, r0, n):
        return pl.ds(pl.multiple_of((zd * 2 + part) * rows + r0, 16), n)

    shifts = [far]
    for d in range(near, 0, -1):
        shifts += [d, -d]
    shifts.append(0)
    slot_of = {s: k for k, s in enumerate(shifts)}
    slot_of[-far] = slot_of[far]

    loads_mine, loads_other = [], []
    for s in shifts:
        zd = at_z(s)
        for part, out in ((other, loads_other), (core, loads_mine)):
            here = block(zd, part, 0, rows)
            out.append(fetch(gu.at[here], g_u.at[here]))
    small = [
        fetch(gn, vin.at[0]), fetch(gb, vin.at[1]), fetch(wn, vw.at[0]), fetch(wb, vw.at[1]),
    ]

    barrier = pltpu.get_barrier_semaphore()
    peers = [{"core": other}, {"z": at_z(1)}, {"z": at_z(-1)}]
    others_y = [lax.rem(y + k, cols) for k in range(1, cols)]
    peers += [{"cols": o} for o in others_y]
    for peer in peers:
        pl.semaphore_signal(barrier, inc=1, device_id=peer, device_id_type=pl.DeviceIdType.MESH)
    pl.semaphore_wait(barrier, len(peers))

    mats = {
        "u": dict(g=g_u, pair=pair_u, rcv=rcv_u, w=w_u, fin=fin_u, full=cu, new=nu, k=0),
        "d": dict(g=g_d, pair=pair_d, rcv=rcv_d, w=w_d, fin=fin_d, full=full_d, new=nd, k=1),
    }

    def swap(name):
        m = mats[name]
        m["swaps"] = []
        for k, s in enumerate(shifts):
            if name == "u":
                loads_other[k].wait()
            zd = at_z(s)
            m["swaps"].append(
                send(m["g"].at[block(zd, other, 0, rows)], m["pair"].at[zd], core=other)
            )
        m["ready"] = set()

    def pair_sum(m, shift, r0, n):
        k = slot_of[shift]
        if k not in m["ready"]:
            if m is mats["u"]:
                loads_mine[k].wait()
            m["swaps"][k].wait_recv()
            m["ready"].add(k)
        zd = at_z(shift)
        mine = m["g"][block(zd, core, r0, n), :].astype(F32)
        return mine + m["pair"][zd, pl.ds(r0, n), :].astype(F32)

    flows = []
    for name, flip in (("u", 0), ("d", 1)):
        for i, (r0, n) in enumerate(cut(rows)):
            reach = (near, far) if (i + flip) % 2 == 0 else (far, near)
            flows.append(dict(m=name, r0=r0, n=n, reach=reach, rs={}, ag={}, to={}))

    def of(name):
        return [f for f in flows if f["m"] == name]

    def scatter(name, step):
        m = mats[name]
        for f in of(name):
            r0, n = f["r0"], f["n"]
            for d, sign in ((1, -1), (0, 1)):
                reach = f["reach"][d]
                if step > reach:
                    continue
                shift = sign * (reach - step + 1)
                if abs(shift) == far:
                    shift = far
                total = pair_sum(m, shift, r0, n)
                if step > 1:
                    f["rs"][d, step - 1].wait_recv()
                    total += m["rcv"][d, step - 2, pl.ds(r0, n), :].astype(F32)
                zd = at_z(shift)
                m["pair"][zd, pl.ds(r0, n), :] = total.astype(BF16)
                f["rs"][d, step] = send(
                    m["pair"].at[zd, pl.ds(r0, n)],
                    m["rcv"].at[d, step - 1, pl.ds(r0, n)],
                    z=at_z(sign),
                )

    def folded(x):
        out = x[:, :LANES]
        for j in range(1, x.shape[1] // LANES):
            out += x[:, j * LANES : (j + 1) * LANES]
        return out

    def share_with_cols(table, k, r0, n):
        return [
            send(table.at[k, y, pl.ds(r0, n)], table.at[k, y, pl.ds(r0, n)], cols=o)
            for o in others_y
        ]

    def finish_sum(name):
        m = mats[name]
        for f in of(name):
            r0, n = f["r0"], f["n"]
            total = pair_sum(m, 0, r0, n)
            for d in (1, 0):
                reach = f["reach"][d]
                f["rs"][d, reach].wait_recv()
                total += m["rcv"][d, reach - 1, pl.ds(r0, n), :].astype(F32)
            mean = total * mean_rate
            m["fin"][pl.ds(r0, n), :] = mean
            slope[m["k"], y, pl.ds(r0, n), :] = folded(mean * mean)
            f["sizes"] = share_with_cols(slope, m["k"], r0, n)

    def size_of(table, k, r0, n):
        total = table[k, 0, pl.ds(r0, n), :]
        for j in range(1, cols):
            total += table[k, j, pl.ds(r0, n), :]
        return jnp.sum(total, axis=1, keepdims=True)

    def update(name):
        m = mats[name]
        for c in m.pop("own_sizes"):
            c.wait_recv()
        for f in of(name):
            r0, n = f["r0"], f["n"]
            for c in f["sizes"]:
                c.wait_recv()
            ratio = jnp.sqrt(size_of(own, m["k"], r0, n)) * lax.rsqrt(
                size_of(slope, m["k"], r0, n) + 1e-06
            )
            new = m["w"][pl.ds(r0, n), :] - RATE * (m["fin"][pl.ds(r0, n), :] * ratio)
            m["new"][pl.ds(r0, n), :] = new
            here = m["full"].at[block(z, core, r0, n)]
            here[...] = new.astype(BF16)
            for d, sign in ((1, -1), (0, 1)):
                f["ag"][d, 1] = send(here, here, z=at_z(sign))
            f["to"][0, 0] = send(here, here, core=other)

    def pass_on(name, step):
        m = mats[name]
        for f in of(name):
            for d, sign in ((1, -1), (0, 1)):
                reach = f["reach"][d]
                if step > reach:
                    continue
                f["ag"][d, step].wait_recv()
                here = m["full"].at[block(at_z(-sign * step), core, f["r0"], f["n"])]
                if step < reach:
                    f["ag"][d, step + 1] = send(here, here, z=at_z(sign))
                f["to"][d, step] = send(here, here, core=other)

    def all_here(name):
        for f in of(name):
            for copy in f["to"].values():
                copy.wait_recv()

    def vectors_out():
        for copy in small:
            copy.wait()
        vplace[...] = jnp.zeros_like(vplace)
        for v in range(2):
            vplace[pl.ds(v, 1), pl.ds(0, rows)] = vw[v]
        placed = pltpu.roll(vplace[...], place * rows, 1)
        for v in range(2):
            vown[v] = placed[v : v + 1, :] - (RATE * mean_rate) * vin[v].astype(F32)
        return send(vown.at[other], vpair, core=other)

    vec = {}

    def vectors_ring(step):
        if step == 1:
            vec["swap"].wait_recv()
            vslot[z] = vown[core] + vpair[...]
        for d, sign in ((1, -1), (0, 1)):
            reach = (near, far)[d]
            if step > 1 and step - 1 <= reach:
                vec[d, step - 1].wait_recv()
            if step <= reach:
                here = vslot.at[at_z(-sign * (step - 1))]
                vec[d, step] = send(here, here, z=at_z(sign))

    def vectors_sum():
        total = vslot[0]
        for k in range(1, ring):
            total += vslot[k]
        vfull[core] = total
        vec["full"] = send(vfull.at[core], vfull.at[core], core=other)

    def vectors_in():
        vec["full"].wait_recv()
        back = lax.rem(ring * 2 - place, ring * 2) * rows
        for v, (c_ref, n_ref) in enumerate(((cn, nn), (cb, nb))):
            c_ref[...] = vfull[v].astype(BF16)
            vplace[pl.ds(v, 1), :] = vfull[v]
        turned = pltpu.roll(vplace[...], back, 1)
        for v, n_ref in enumerate((nn, nb)):
            n_ref[...] = turned[v : v + 1, :rows]

    def turn_in():
        load_raw.wait()

        def slab(j, _):
            here = pl.ds(pl.multiple_of(j * LANES, LANES), LANES)
            g_d[here, :] = raw[:, here].T
            return 0

        lax.fori_loop(0, ring * 2 * rows // LANES, slab, 0)

    def own_sizes():
        for copy in load_w:
            copy.wait()
        for name in ("u", "d"):
            m = mats[name]
            w = m["w"][...]
            own[m["k"], y] = folded(w * w)
            m["own_sizes"] = share_with_cols(own, m["k"], 0, rows)

    swap("u")
    load_raw = fetch(gd, raw)
    load_w = [fetch(wu, w_u), fetch(wd, w_d)]
    steps = far
    scatter("u", 1)
    vec["swap"] = vectors_out()
    turn_in()
    swap("d")
    vectors_ring(1)
    own_sizes()
    for s in range(2, steps):
        scatter("u", s)
        vectors_ring(s)
    scatter("d", 1)
    if steps > 1:
        scatter("u", steps)
        vectors_ring(steps)
        scatter("d", 2)
    finish_sum("u")
    for s in range(3, steps + 1):
        scatter("d", s)
    vectors_ring(steps + 1)
    vectors_sum()
    update("u")
    finish_sum("d")
    pass_on("u", 1)
    update("d")
    vectors_in()
    for s in range(2, steps + 1):
        pass_on("u", s)
        pass_on("d", s - 1)
    pass_on("d", steps)
    all_here("d")
    all_here("u")
    for copy in sent:
        copy.wait_send()


def put(cu, full_d, cn, cb, nu, nd, nn, nb, cu_o, cd_o, cn_o, cb_o, nu_o, nd_o, nn_o, nb_o, turned, sems):
    copies = []

    def write(src, dst):
        copies.append(pltpu.make_async_copy(src, dst, sems.at[len(copies)]))
        copies[-1].start()

    wide = turned.shape[0]
    for r in range(0, wide, LANES):
        here = pl.ds(r, LANES)
        turned[here, :] = full_d[:, here].T
        write(turned.at[here], cd_o.at[here])
        part = pl.ds(r * cu.shape[0] // wide, LANES * cu.shape[0] // wide)
        write(cu.at[part], cu_o.at[part])
    for src, dst in ((nu, nu_o), (nd, nd_o), (nn, nn_o), (nb, nb_o)):
        write(src, dst)
    cn_o[...] = cn[0, :]
    cb_o[...] = cb[0, :]
    for copy in copies:
        copy.wait()


def per_device(ring, cols, grad_up, grad_down, grad_norm, grad_bias, *weights):
    weight_up, weight_down, weight_norm, weight_bias = weights
    rows, wide = weight_up.shape
    total = ring * 2 * rows
    any_spec = pl.BlockSpec(memory_space=pl.ANY)
    vmem = pl.BlockSpec(memory_space=pltpu.VMEM)
    shape = jax.ShapeDtypeStruct
    outs = (
        shape((total, wide), BF16), shape((wide, total), BF16),
        shape((1, total), BF16), shape((1, total), BF16),
        shape((rows, wide), F32), shape((rows, wide), F32),
        shape((1, rows), F32), shape((1, rows), F32),
    )
    far = ring // 2
    scratch = [
        pltpu.VMEM((wide, total), BF16),
        pltpu.VMEM((total, wide), BF16), pltpu.VMEM((total, wide), BF16),
        pltpu.VMEM((ring, rows, wide), BF16), pltpu.VMEM((ring, rows, wide), BF16),
        pltpu.VMEM((2, far, rows, wide), BF16), pltpu.VMEM((2, far, rows, wide), BF16),
        pltpu.VMEM((rows, wide), F32), pltpu.VMEM((rows, wide), F32),
        pltpu.VMEM((rows, wide), F32), pltpu.VMEM((rows, wide), F32),
        pltpu.VMEM((2, cols, rows, LANES), F32), pltpu.VMEM((2, cols, rows, LANES), F32),
        pltpu.VMEM((2, 1, total), BF16), pltpu.VMEM((2, 1, rows), F32),
        pltpu.VMEM((8, total), F32), pltpu.VMEM((2, 1, total), F32),
        pltpu.VMEM((1, total), F32), pltpu.VMEM((ring, 1, total), F32),
        pltpu.VMEM((2, 1, total), F32),
        pltpu.SemaphoreType.DMA((448,)),
    ]
    got = pl.pallas_call(
        functools.partial(kernel, (ring, cols, rows, wide)),
        out_shape=[
            pltpu.VMEM((total, wide) if k == 1 else o.shape, o.dtype) for k, o in enumerate(outs)
        ],
        in_specs=[pl.BlockSpec(memory_space=pltpu.HBM)] * 8,
        out_specs=[vmem] * 8,
        scratch_shapes=scratch,
        compiler_params=pltpu.CompilerParams(
            collective_id=0, has_side_effects=True, vmem_limit_bytes=VL * 2**20
        ),
        name="step",
    )(
        *(
            pltpu.with_memory_space_constraint(a, pltpu.HBM)
            for a in (
                grad_up[0], grad_down[0], grad_norm, grad_bias,
                weight_up, weight_down.T, weight_norm[None], weight_bias[None],
            )
        )
    )
    flat = shape((total,), BF16)
    got = pl.pallas_call(
        put,
        out_shape=(*outs[:2], flat, flat, *outs[4:]),
        in_specs=[vmem] * 8,
        out_specs=[any_spec] * 2 + [vmem] * 2 + [any_spec] * 4,
        scratch_shapes=[
            pltpu.VMEM((wide, total), BF16),
            pltpu.SemaphoreType.DMA((2 * wide // LANES + 4,)),
        ],
        compiler_params=pltpu.CompilerParams(vmem_limit_bytes=8 * 2**20),
        name="put",
    )(*got)
    copy_up, copy_down, copy_norm, copy_bias, new_up, new_down, new_norm, new_bias = got
    return (
        copy_up, copy_down, copy_norm, copy_bias,
        new_up, new_down.T, new_norm[0], new_bias[0],
    )


def solution(mesh):
    ring, cols = mesh.shape["batch"] // 2, mesh.shape["cols"]
    finer = Mesh(mesh.devices.reshape(mesh.shape["ens"], ring, 2, cols), AXES)
    batch = ("z", "core")
    all_of = ("ens", "z", "core")
    placed = (
        P(all_of, None, "cols"), P(all_of, "cols", None), P(all_of, None), P(all_of, None),
        P(all_of, "cols"), P(("ens", "cols"), batch), P(all_of), P(all_of),
    )
    return jax.shard_map(
        functools.partial(per_device, ring, cols),
        mesh=finer,
        in_specs=placed,
        out_specs=(
            P("ens", "cols"), P(("ens", "cols"), None), P("ens"), P("ens"),
            P(all_of, "cols"), P(("ens", "cols"), batch), P(all_of), P(all_of),
        ),
        check_vma=False,
    )
```

```python
import functools

import jax
import jax.numpy as jnp
from jax import lax
from jax.experimental import pallas as pl
from jax.experimental.pallas import tpu as pltpu
from jax.sharding import Mesh
from jax.sharding import PartitionSpec as P

AXES = ("ens", "z", "core", "cols")
RATE = 0.4
VL = 52
LANES = 128
F32 = jnp.float32
BF16 = jnp.bfloat16


def cut(rows):
    parts, at = [], 0
    for size in (32, 32, 16):
        if at < rows:
            parts.append((at, min(size, rows - at)))
            at += size
    return parts


def kernel(
    dims,
    gu, gd, gn, gb, wu, wd, wn, wb,
    cu, full_d, cn, cb, nu, nd, nn, nb,
    raw, g_u, g_d, pair_u, pair_d, rcv_u, rcv_d, w_u, w_d, fin_u, fin_d,
    slope, own, vin, vw, vplace, vown, vpair, vslot, vfull, sems, gates,
):
    ring, cols, rows, wide = dims
    z, core, y = lax.axis_index("z"), lax.axis_index("core"), lax.axis_index("cols")
    other = 1 - core
    far, near = ring // 2, ring - 1 - ring // 2
    mean_rate = (ring * 2) ** -0.5
    place = z * 2 + core
    count = [0]
    sent = []

    def new_sem():
        count[0] += 1
        return sems.at[count[0] - 1]

    def at_z(shift):
        return lax.rem(z + (shift + ring), ring)

    def fetch(src, dst):
        copy = pltpu.make_async_copy(src, dst, new_sem())
        copy.start()
        return copy

    def send(src, dst, **where):
        copy = pltpu.make_async_remote_copy(
            src_ref=src, dst_ref=dst, send_sem=new_sem(), recv_sem=new_sem(),
            device_id=where, device_id_type=pl.DeviceIdType.MESH,
        )
        copy.start()
        sent.append(copy)
        return copy

    def block(zd, part, r0, n):
        return pl.ds(pl.multiple_of((zd * 2 + part) * rows + r0, 16), n)

    shifts = [far]
    for d in range(near, 0, -1):
        shifts += [d, -d]
    shifts.append(0)
    slot_of = {s: k for k, s in enumerate(shifts)}
    slot_of[-far] = slot_of[far]

    loads_mine, loads_other = [], []
    first = 3

    def load(part, out, which):
        for s in which:
            here = block(at_z(s), part, 0, rows)
            out.append(fetch(gu.at[here], g_u.at[here]))

    load(other, loads_other, shifts[:first])
    load(core, loads_mine, shifts[:first])
    load(other, loads_other, shifts[first:])
    load(core, loads_mine, shifts[first:])
    load_raw = fetch(gd, raw)
    load_w = [fetch(wu, w_u), fetch(wd, w_d)]
    small = [
        fetch(gn, vin.at[0]), fetch(gb, vin.at[1]), fetch(wn, vw.at[0]), fetch(wb, vw.at[1]),
    ]

    barrier = pltpu.get_barrier_semaphore()
    others_y = [lax.rem(y + k, cols) for k in range(1, cols)]

    def signal(sem, **where):
        pl.semaphore_signal(sem, inc=1, device_id=where, device_id_type=pl.DeviceIdType.MESH)

    for shift in (1, -1):
        signal(barrier, z=at_z(shift), core=1)
    for o in others_y:
        signal(barrier, cols=o, core=0)

    @pl.when(core == 0)
    def _():
        signal(barrier, core=1)
        pl.semaphore_wait(gates.at[0], 1)

    @pl.when(core == 1)
    def _():
        pl.semaphore_wait(barrier, 5)
        signal(gates.at[0], core=0)

    def meet_columns():
        @pl.when(core == 0)
        def _():
            pl.semaphore_wait(barrier, 2 * len(others_y))
            signal(gates.at[1], core=1)

        @pl.when(core == 1)
        def _():
            pl.semaphore_wait(gates.at[1], 1)

    mats = {
        "u": dict(g=g_u, pair=pair_u, rcv=rcv_u, w=w_u, fin=fin_u, full=cu, new=nu, k=0, swaps={}, ready=set(), mine=set()),
        "d": dict(g=g_d, pair=pair_d, rcv=rcv_d, w=w_d, fin=fin_d, full=full_d, new=nd, k=1, swaps={}, ready=set(), mine=set()),
    }

    flows = []
    for name, flip in (("u", 0), ("d", 1)):
        for i, (r0, n) in enumerate(cut(rows)):
            reach = (near, far) if (i + flip) % 2 == 0 else (far, near)
            flows.append(dict(m=name, r0=r0, n=n, reach=reach, rs={}, ag={}, to={}))

    def of(name):
        return [f for f in flows if f["m"] == name]

    def swap(name, begin=0, end=None):
        m = mats[name]
        for k, s in list(enumerate(shifts))[begin:end]:
            if name == "u":
                loads_other[k].wait()
            zd = at_z(s)
            m["swaps"][k, 0] = send(
                m["g"].at[block(zd, other, 0, rows)], m["pair"].at[zd], core=other
            )

    def swap_first(name):
        m = mats[name]
        for copy in loads_other[:first]:
            copy.wait()
        now, later = [], []
        for f in of(name):
            early = {far, f["reach"][0] if f["reach"][0] != far else -f["reach"][1]}
            for k, s in enumerate(shifts[:first]):
                (now if s in early else later).append((k, s, f["r0"], f["n"]))
        for k, s, r0, n in now + later:
            zd = at_z(s)
            m["swaps"][k, r0] = send(
                m["g"].at[block(zd, other, r0, n)], m["pair"].at[zd, pl.ds(r0, n)], core=other
            )

    def pair_sum(m, shift, r0, n):
        k = slot_of[shift]
        if m is mats["u"] and k not in m["mine"]:
            loads_mine[k].wait()
            m["mine"].add(k)
        key = (k, r0) if (k, r0) in m["swaps"] else (k, 0)
        if key not in m["ready"]:
            m["swaps"][key].wait_recv()
            m["ready"].add(key)
        zd = at_z(shift)
        mine = m["g"][block(zd, core, r0, n), :].astype(F32)
        return mine + m["pair"][zd, pl.ds(r0, n), :].astype(F32)

    def scatter(name, step):
        m = mats[name]
        for f in of(name):
            r0, n = f["r0"], f["n"]
            for d, sign in ((1, -1), (0, 1)):
                reach = f["reach"][d]
                if step > reach:
                    continue
                shift = sign * (reach - step + 1)
                if abs(shift) == far:
                    shift = far
                total = pair_sum(m, shift, r0, n)
                if step > 1:
                    f["rs"][d, step - 1].wait_recv()
                    total += m["rcv"][d, step - 2, pl.ds(r0, n), :].astype(F32)
                zd = at_z(shift)
                m["pair"][zd, pl.ds(r0, n), :] = total.astype(BF16)
                f["rs"][d, step] = send(
                    m["pair"].at[zd, pl.ds(r0, n)],
                    m["rcv"].at[d, step - 1, pl.ds(r0, n)],
                    z=at_z(sign),
                )

    def folded(x):
        out = x[:, :LANES]
        for j in range(1, x.shape[1] // LANES):
            out += x[:, j * LANES : (j + 1) * LANES]
        return out

    def share_with_cols(table, k, r0, n):
        return [
            send(table.at[k, y, pl.ds(r0, n)], table.at[k, y, pl.ds(r0, n)], cols=o)
            for o in others_y
        ]

    def finish_sum(name):
        m = mats[name]
        for f in of(name):
            r0, n = f["r0"], f["n"]
            total = pair_sum(m, 0, r0, n)
            for d in (1, 0):
                reach = f["reach"][d]
                f["rs"][d, reach].wait_recv()
                total += m["rcv"][d, reach - 1, pl.ds(r0, n), :].astype(F32)
            mean = total * mean_rate
            m["fin"][pl.ds(r0, n), :] = mean
            slope[m["k"], y, pl.ds(r0, n), :] = folded(mean * mean)
            f["sizes"] = share_with_cols(slope, m["k"], r0, n)

    def size_of(table, k, r0, n):
        total = table[k, 0, pl.ds(r0, n), :]
        for j in range(1, cols):
            total += table[k, j, pl.ds(r0, n), :]
        return jnp.sum(total, axis=1, keepdims=True)

    def update(name):
        m = mats[name]
        for c in m.pop("own_sizes"):
            c.wait_recv()
        for f in of(name):
            r0, n = f["r0"], f["n"]
            for c in f["sizes"]:
                c.wait_recv()
            ratio = jnp.sqrt(size_of(own, m["k"], r0, n)) * lax.rsqrt(
                size_of(slope, m["k"], r0, n) + 1e-06
            )
            new = m["w"][pl.ds(r0, n), :] - RATE * (m["fin"][pl.ds(r0, n), :] * ratio)
            m["new"][pl.ds(r0, n), :] = new
            here = m["full"].at[block(z, core, r0, n)]
            here[...] = new.astype(BF16)
            for d, sign in ((1, -1), (0, 1)):
                f["ag"][d, 1] = send(here, here, z=at_z(sign))
            f["to"][0, 0] = send(here, here, core=other)

    def pass_on(name, step):
        m = mats[name]
        for f in of(name):
            for d, sign in ((1, -1), (0, 1)):
                reach = f["reach"][d]
                if step > reach:
                    continue
                f["ag"][d, step].wait_recv()
                here = m["full"].at[block(at_z(-sign * step), core, f["r0"], f["n"])]
                if step < reach:
                    f["ag"][d, step + 1] = send(here, here, z=at_z(sign))
                f["to"][d, step] = send(here, here, core=other)

    def all_here(name):
        for f in of(name):
            for copy in f["to"].values():
                copy.wait_recv()

    def vectors_out():
        for copy in small:
            copy.wait()
        vplace[...] = jnp.zeros_like(vplace)
        for v in range(2):
            vplace[pl.ds(v, 1), pl.ds(0, rows)] = vw[v]
        placed = pltpu.roll(vplace[...], place * rows, 1)
        for v in range(2):
            vown[v] = placed[v : v + 1, :] - (RATE * mean_rate) * vin[v].astype(F32)
        return send(vown.at[other], vpair, core=other)

    vec = {}

    def vectors_ring(step):
        if step == 1:
            vec["swap"].wait_recv()
            vslot[z] = vown[core] + vpair[...]
        for d, sign in ((1, -1), (0, 1)):
            reach = (near, far)[d]
            if step > 1 and step - 1 <= reach:
                vec[d, step - 1].wait_recv()
            if step <= reach:
                here = vslot.at[at_z(-sign * (step - 1))]
                vec[d, step] = send(here, here, z=at_z(sign))

    def vectors_sum():
        total = vslot[0]
        for k in range(1, ring):
            total += vslot[k]
        vfull[core] = total
        vec["full"] = send(vfull.at[core], vfull.at[core], core=other)

    def vectors_in():
        vec["full"].wait_recv()
        back = lax.rem(ring * 2 - place, ring * 2) * rows
        for v, (c_ref, n_ref) in enumerate(((cn, nn), (cb, nb))):
            c_ref[...] = vfull[v].astype(BF16)
            vplace[pl.ds(v, 1), :] = vfull[v]
        turned = pltpu.roll(vplace[...], back, 1)
        for v, n_ref in enumerate((nn, nb)):
            n_ref[...] = turned[v : v + 1, :rows]

    def turn_in():
        load_raw.wait()

        def slab(j, _):
            here = pl.ds(pl.multiple_of(j * LANES, LANES), LANES)
            g_d[here, :] = raw[:, here].T
            return 0

        lax.fori_loop(0, ring * 2 * rows // LANES, slab, 0)

    def own_sizes():
        for copy in load_w:
            copy.wait()
        for name in ("u", "d"):
            m = mats[name]
            w = m["w"][...]
            own[m["k"], y] = folded(w * w)
            m["own_sizes"] = share_with_cols(own, m["k"], 0, rows)

    swap_first("u")
    steps = far
    scatter("u", 1)
    swap("u", first)
    vec["swap"] = vectors_out()
    turn_in()
    swap("d")
    vectors_ring(1)
    meet_columns()
    own_sizes()
    scatter("u", 2)
    vectors_ring(2)
    scatter("d", 1)
    scatter("u", 3)
    vectors_ring(3)
    scatter("d", 2)
    scatter("u", 4)
    vectors_ring(4)
    scatter("d", 3)
    finish_sum("u")
    scatter("d", 4)
    vectors_ring(5)
    vectors_sum()
    update("u")
    finish_sum("d")
    pass_on("u", 1)
    update("d")
    vectors_in()
    pass_on("u", 2)
    pass_on("d", 1)
    pass_on("d", 2)
    pass_on("u", 3)
    pass_on("d", 3)
    pass_on("u", 4)
    pass_on("d", 4)
    all_here("d")
    all_here("u")
    for copy in sent:
        copy.wait_send()


def put(cu, full_d, cn, cb, nu, nd, nn, nb, cu_o, cd_o, cn_o, cb_o, nu_o, nd_o, nn_o, nb_o, turned, line_n, line_b, sems):
    copies = []

    def write(src, dst):
        copies.append(pltpu.make_async_copy(src, dst, sems.at[len(copies)]))
        copies[-1].start()

    wide = turned.shape[0]
    for r in range(0, wide, LANES):
        here = pl.ds(r, LANES)
        turned[here, :] = full_d[:, here].T
        write(turned.at[here], cd_o.at[here])
        part = pl.ds(r * cu.shape[0] // wide, LANES * cu.shape[0] // wide)
        write(cu.at[part], cu_o.at[part])
    for src, dst in ((nu, nu_o), (nd, nd_o), (nn, nn_o), (nb, nb_o)):
        write(src, dst)
    for src, line, dst in ((cn, line_n, cn_o), (cb, line_b, cb_o)):
        line[...] = src[0, :]
        write(line, dst)
    for copy in copies:
        copy.wait()


def per_device(ring, cols, grad_up, grad_down, grad_norm, grad_bias, *weights):
    weight_up, weight_down, weight_norm, weight_bias = weights
    rows, wide = weight_up.shape
    total = ring * 2 * rows
    any_spec = pl.BlockSpec(memory_space=pl.ANY)
    vmem = pl.BlockSpec(memory_space=pltpu.VMEM)
    shape = jax.ShapeDtypeStruct
    outs = (
        shape((total, wide), BF16), shape((wide, total), BF16),
        shape((1, total), BF16), shape((1, total), BF16),
        shape((rows, wide), F32), shape((rows, wide), F32),
        shape((1, rows), F32), shape((1, rows), F32),
    )
    far = ring // 2
    scratch = [
        pltpu.VMEM((wide, total), BF16),
        pltpu.VMEM((total, wide), BF16), pltpu.VMEM((total, wide), BF16),
        pltpu.VMEM((ring, rows, wide), BF16), pltpu.VMEM((ring, rows, wide), BF16),
        pltpu.VMEM((2, far, rows, wide), BF16), pltpu.VMEM((2, far, rows, wide), BF16),
        pltpu.VMEM((rows, wide), F32), pltpu.VMEM((rows, wide), F32),
        pltpu.VMEM((rows, wide), F32), pltpu.VMEM((rows, wide), F32),
        pltpu.VMEM((2, cols, rows, LANES), F32), pltpu.VMEM((2, cols, rows, LANES), F32),
        pltpu.VMEM((2, 1, total), BF16), pltpu.VMEM((2, 1, rows), F32),
        pltpu.VMEM((8, total), F32), pltpu.VMEM((2, 1, total), F32),
        pltpu.VMEM((1, total), F32), pltpu.VMEM((ring, 1, total), F32),
        pltpu.VMEM((2, 1, total), F32),
        pltpu.SemaphoreType.DMA((480,)),
        pltpu.SemaphoreType.REGULAR((2,)),
    ]
    got = pl.pallas_call(
        functools.partial(kernel, (ring, cols, rows, wide)),
        out_shape=[
            pltpu.VMEM((total, wide) if k == 1 else o.shape, o.dtype) for k, o in enumerate(outs)
        ],
        in_specs=[pl.BlockSpec(memory_space=pltpu.HBM)] * 8,
        out_specs=[vmem] * 8,
        scratch_shapes=scratch,
        compiler_params=pltpu.CompilerParams(
            collective_id=0, has_side_effects=True, vmem_limit_bytes=VL * 2**20
        ),
        name="step",
    )(
        *(
            pltpu.with_memory_space_constraint(a, pltpu.HBM)
            for a in (
                grad_up[0], grad_down[0], grad_norm, grad_bias,
                weight_up, weight_down.T, weight_norm[None], weight_bias[None],
            )
        )
    )
    flat = shape((total,), BF16)
    got = pl.pallas_call(
        put,
        out_shape=(*outs[:2], flat, flat, *outs[4:]),
        in_specs=[vmem] * 8,
        out_specs=[any_spec] * 8,
        scratch_shapes=[
            pltpu.VMEM((wide, total), BF16),
            pltpu.VMEM((total,), BF16), pltpu.VMEM((total,), BF16),
            pltpu.SemaphoreType.DMA((2 * wide // LANES + 6,)),
        ],
        compiler_params=pltpu.CompilerParams(vmem_limit_bytes=8 * 2**20),
        name="put",
    )(*got)
    copy_up, copy_down, copy_norm, copy_bias, new_up, new_down, new_norm, new_bias = got
    return (
        copy_up, copy_down, copy_norm, copy_bias,
        new_up, new_down.T, new_norm[0], new_bias[0],
    )


def solution(mesh):
    ring, cols = mesh.shape["batch"] // 2, mesh.shape["cols"]
    finer = Mesh(mesh.devices.reshape(mesh.shape["ens"], ring, 2, cols), AXES)
    batch = ("z", "core")
    all_of = ("ens", "z", "core")
    placed = (
        P(all_of, None, "cols"), P(all_of, "cols", None), P(all_of, None), P(all_of, None),
        P(all_of, "cols"), P(("ens", "cols"), batch), P(all_of), P(all_of),
    )
    return jax.shard_map(
        functools.partial(per_device, ring, cols),
        mesh=finer,
        in_specs=placed,
        out_specs=(
            P("ens", "cols"), P(("ens", "cols"), None), P("ens"), P("ens"),
            P(all_of, "cols"), P(("ens", "cols"), batch), P(all_of), P(all_of),
        ),
        check_vma=False,
    )
```
